8 devices in a mesh: gp: 8 (over z, y, x, core).
Axes of the slice: x: 2, y: 2, z: 1, core: 2. Of those that a mesh axis runs over, the one named last changes fastest.
Arguments:
- grid_in: bfloat16 [12288, 272], P('gp')
- mesh_static: bfloat16 [1024, 3], P('gp')
- edge_static: bfloat16 [18432, 4], P('gp')
- send_rows: int32 [64, 192], P('gp')
- edge_src: int32 [18432], P('gp')
- edge_dst: int32 [18432], P('gp')
- w_grid_in: bfloat16 [272, 512], replicated
- w_mesh_in: bfloat16 [3, 512], replicated
- w_edge_in: bfloat16 [4, 512], replicated
- w_edge_up: bfloat16 [1536, 512], replicated
- w_mesh_up: bfloat16 [1024, 512], replicated
- w_grid_up: bfloat16 [512, 512], replicated
- w_second: bfloat16 [6, 512, 512], replicated
- vectors: float32 [6, 4, 512], replicated
- d_mesh_out: bfloat16 [1024, 512], P('gp')
- d_grid_out: bfloat16 [12288, 512], P('gp')
Outputs:
- output 1: bfloat16 [1024, 512], P('gp')
- output 2: bfloat16 [12288, 512], P('gp')
- output 3: float32 [12288, 272], P('gp')
- output 4: float32 [272, 512], replicated
- output 5: float32 [3, 512], replicated
- output 6: float32 [4, 512], replicated
- output 7: float32 [1536, 512], replicated
- output 8: float32 [1024, 512], replicated
- output 9: float32 [512, 512], replicated
- output 10: float32 [6, 512, 512], replicated
- output 11: float32 [6, 4, 512], replicated
All inputs are finite; a program needn't handle non-finite values.
Results may differ from the reference program's by a relative error of at most 0.0196952.
Values are sent between devices in bfloat16 or wider.
A program may use at most 1 GiB of HBM per device.

```python
import jax
import jax.numpy as jnp
from jax import lax

NUM_PARTS = 8
GRID_DEV = 1536
MESH_DEV = 128
FEATURES = 272
LATENT = 512
MESH_FEAT = 3
EDGE_FEAT = 4
EDGE_DEV = 2304
SLOT_CAP = 192
GRID_ALL = NUM_PARTS * GRID_DEV
MESH_ALL = NUM_PARTS * MESH_DEV
EDGE_ALL = NUM_PARTS * EDGE_DEV
LN_EPS = 1e-5


def draw_indices(key):
    sub_keys = jax.random.split(key, 5)
    band_ids = jnp.arange(NUM_PARTS)
    polar_band = (band_ids == 0) | (band_ids == NUM_PARTS - 1)
    low_cap = SLOT_CAP // 4
    counts = low_cap + jax.random.randint(sub_keys[0], (NUM_PARTS, NUM_PARTS), 0, SLOT_CAP - low_cap + 1, dtype=jnp.int32)
    counts = jnp.where(polar_band[:, None], SLOT_CAP, counts)
    send_rows = jax.random.randint(sub_keys[1], (NUM_PARTS * NUM_PARTS, SLOT_CAP), 0, GRID_DEV, dtype=jnp.int32)
    slot_valid = jnp.arange(SLOT_CAP)[None, None, :] < counts.T[:, :, None]
    buf_len = NUM_PARTS * SLOT_CAP
    slot_valid = slot_valid.reshape(NUM_PARTS, buf_len)
    order_key = jnp.where(slot_valid, 0, buf_len) + jnp.arange(buf_len)[None, :]
    slot_order = jnp.argsort(order_key, axis=1).astype(jnp.int32)
    n_valid = jnp.sum(slot_valid, axis=1).astype(jnp.int32)
    edge_ids = jnp.arange(EDGE_DEV, dtype=jnp.int32)[None, :]
    slot_pick = jax.random.randint(sub_keys[2], (NUM_PARTS, EDGE_DEV), 0, n_valid[:, None], dtype=jnp.int32)
    slot_pick = jnp.where(edge_ids < n_valid[:, None], edge_ids, slot_pick)
    edge_src = jnp.take_along_axis(slot_order, slot_pick, axis=1)
    dst_draw = jax.random.randint(sub_keys[3], (NUM_PARTS, EDGE_DEV), 0, MESH_DEV, dtype=jnp.int32)
    dst_draw = jnp.where(edge_ids < MESH_DEV, edge_ids, dst_draw)
    edge_dst = jax.random.permutation(sub_keys[4], dst_draw, axis=1, independent=True)
    return send_rows, edge_src.reshape(-1).astype(jnp.int32), edge_dst.reshape(-1).astype(jnp.int32)


def weight_draw(key, shape, fan_in):
    return (jax.random.normal(key, shape, jnp.float32) * fan_in ** -0.5).astype(jnp.bfloat16)


def setup_inputs(seed: int = 0) -> dict:
    key = jax.random.key(seed)
    sub_keys = jax.random.split(key, 16)
    send_rows, edge_src, edge_dst = draw_indices(sub_keys[0])
    grid_in = jax.random.normal(sub_keys[1], (GRID_ALL, FEATURES), jnp.float32)
    lat_draw = jax.random.uniform(sub_keys[2], (MESH_ALL,), jnp.float32, -1.5, 1.5)
    lon_draw = jax.random.uniform(sub_keys[3], (MESH_ALL,), jnp.float32, 0.0, 6.28)
    mesh_static = jnp.stack([jnp.cos(lat_draw), jnp.sin(lon_draw), jnp.cos(lon_draw)], axis=1)
    offsets = 0.5 * jax.random.normal(sub_keys[4], (EDGE_ALL, EDGE_FEAT - 1), jnp.float32)
    lengths = jnp.sqrt(jnp.sum(offsets * offsets, axis=1, keepdims=True))
    edge_static = jnp.concatenate([lengths, offsets], axis=1)
    vec_noise = jax.random.normal(sub_keys[12], (6, 4, LATENT), jnp.float32)
    vec_scale = jnp.array([0.3, 0.3, 0.2, 0.3], jnp.float32)
    vec_shift = jnp.array([0.0, 0.0, 1.0, 0.0], jnp.float32)
    vectors = vec_noise * vec_scale[None, :, None] + vec_shift[None, :, None]
    return {
        'grid_in': grid_in.astype(jnp.bfloat16),
        'mesh_static': mesh_static.astype(jnp.bfloat16),
        'edge_static': edge_static.astype(jnp.bfloat16),
        'send_rows': send_rows,
        'edge_src': edge_src,
        'edge_dst': edge_dst,
        'w_grid_in': weight_draw(sub_keys[5], (FEATURES, LATENT), FEATURES),
        'w_mesh_in': weight_draw(sub_keys[6], (MESH_FEAT, LATENT), MESH_FEAT),
        'w_edge_in': weight_draw(sub_keys[7], (EDGE_FEAT, LATENT), EDGE_FEAT),
        'w_edge_up': weight_draw(sub_keys[8], (3 * LATENT, LATENT), 3 * LATENT),
        'w_mesh_up': weight_draw(sub_keys[9], (2 * LATENT, LATENT), 2 * LATENT),
        'w_grid_up': weight_draw(sub_keys[10], (LATENT, LATENT), LATENT),
        'w_second': weight_draw(sub_keys[11], (6, LATENT, LATENT), LATENT),
        'vectors': vectors,
        'd_mesh_out': jax.random.normal(sub_keys[13], (MESH_ALL, LATENT), jnp.float32).astype(jnp.bfloat16),
        'd_grid_out': jax.random.normal(sub_keys[14], (GRID_ALL, LATENT), jnp.float32).astype(jnp.bfloat16),
    }


def mlp_tail(pre_act, w_two, vec_rows):
    pre_bias = pre_act + vec_rows[0]
    hidden = jax.nn.silu(pre_bias).astype(jnp.bfloat16)
    out_lin = jnp.dot(hidden, w_two, preferred_element_type=jnp.float32) + vec_rows[1]
    centered = out_lin - jnp.mean(out_lin, axis=-1, keepdims=True)
    inv_std = lax.rsqrt(jnp.mean(centered * centered, axis=-1, keepdims=True) + LN_EPS)
    return centered * inv_std * vec_rows[2] + vec_rows[3]


def first_layer(feat_in, w_first):
    return jnp.dot(feat_in, w_first, preferred_element_type=jnp.float32)


def reference(grid_in, mesh_static, edge_static, send_rows, edge_src, edge_dst, w_grid_in, w_mesh_in, w_edge_in, w_edge_up, w_mesh_up, w_grid_up, w_second, vectors, d_mesh_out, d_grid_out):
    edge_part = jnp.arange(EDGE_ALL, dtype=jnp.int32) // EDGE_DEV
    band_ids = edge_src // SLOT_CAP
    sender = band_ids * GRID_DEV + send_rows[band_ids * NUM_PARTS + edge_part, edge_src % SLOT_CAP]
    receiver = edge_part * MESH_DEV + edge_dst

    def forward(grid_x, wg_in, wm_in, we_in, we_up, wm_up, wg_up, w_two_all, vec_all):
        grid_lat = mlp_tail(first_layer(grid_x, wg_in), w_two_all[0], vec_all[0]).astype(jnp.bfloat16)
        mesh_lat = mlp_tail(first_layer(mesh_static, wm_in), w_two_all[1], vec_all[1]).astype(jnp.bfloat16)
        edge_lat = mlp_tail(first_layer(edge_static, we_in), w_two_all[2], vec_all[2]).astype(jnp.bfloat16)
        edge_cat = jnp.concatenate([edge_lat, jnp.take(grid_lat, sender, axis=0), jnp.take(mesh_lat, receiver, axis=0)], axis=1)
        edge_new = (edge_lat.astype(jnp.float32) + mlp_tail(first_layer(edge_cat, we_up), w_two_all[3], vec_all[3])).astype(jnp.bfloat16)
        agg_sum = jax.ops.segment_sum(edge_new.astype(jnp.float32), receiver, num_segments=MESH_ALL)
        mesh_cat = jnp.concatenate([mesh_lat, agg_sum.astype(jnp.bfloat16)], axis=1)
        mesh_out = (mesh_lat.astype(jnp.float32) + mlp_tail(first_layer(mesh_cat, wm_up), w_two_all[4], vec_all[4])).astype(jnp.bfloat16)
        grid_out = (grid_lat.astype(jnp.float32) + mlp_tail(first_layer(grid_lat, wg_up), w_two_all[5], vec_all[5])).astype(jnp.bfloat16)
        return mesh_out, grid_out

    fwd_outs, pull_back = jax.vjp(forward, grid_in, w_grid_in, w_mesh_in, w_edge_in, w_edge_up, w_mesh_up, w_grid_up, w_second, vectors)
    all_grads = pull_back((d_mesh_out, d_grid_out))
    return (fwd_outs[0], fwd_outs[1], all_grads[0].astype(jnp.float32), all_grads[1].astype(jnp.float32), all_grads[2].astype(jnp.float32), all_grads[3].astype(jnp.float32), all_grads[4].astype(jnp.float32), all_grads[5].astype(jnp.float32), all_grads[6].astype(jnp.float32), all_grads[7].astype(jnp.float32), all_grads[8].astype(jnp.float32))
```

```python
import jax
import jax.numpy as jnp
from jax import lax
from jax.experimental import pallas as pl
from jax.experimental.pallas import tpu as pltpu
from jax.sharding import PartitionSpec as P

LN_EPS = 1e-5
AXIS_NAME = 'gp'
MESH_ID = pl.DeviceIdType.MESH
BF = jnp.bfloat16
F32 = jnp.float32


def chunked(rows, step, fn):
    lax.fori_loop(0, rows // step, lambda i, c: (fn(i * step), c)[1], 0)


def row_slice(start, size):
    return pl.ds(pl.multiple_of(start, 16), size)


def place():
    me = lax.axis_index(AXIS_NAME)
    core, xpos, ypos = me % 2, (me // 2) % 2, me // 4
    return me, core, xpos, ypos, me + 1 - 2 * core, me + 2 - 4 * xpos, me + 4 - 8 * ypos


def remote(src, dst, sems, idx, dev):
    return pltpu.make_async_remote_copy(src_ref=src, dst_ref=dst, send_sem=sems.at[0, idx], recv_sem=sems.at[1, idx],
                                        device_id=(dev,), device_id_type=MESH_ID)


def barrier_signal():
    me = lax.axis_index(AXIS_NAME)
    barrier = pltpu.get_barrier_semaphore()
    for step in range(1, 8):
        pl.semaphore_signal(barrier, inc=1, device_id=((me + step) % 8,), device_id_type=MESH_ID)


def barrier_wait():
    pl.semaphore_wait(pltpu.get_barrier_semaphore(), 7)


def flip(me, k):
    core, xpos, ypos = me % 2, (me // 2) % 2, me // 4
    core = 1 - core if k & 1 else core
    xpos = 1 - xpos if k & 2 else xpos
    ypos = 1 - ypos if k & 4 else ypos
    return core + 2 * xpos + 4 * ypos


NUM_SEMS = 10


def reduce_steps(grad, out, half_in, mid, last, sems):
    rows = grad.shape[0]
    r2, r4, r8, r16 = rows // 2, rows // 4, rows // 8, rows // 16
    _, core, xpos, ypos, pc, px, py = place()
    sent = []

    def go(src, dst, idx, dev):
        copy = remote(src, dst, sems, idx, dev)
        copy.start()
        sent.append(copy)
        return copy

    first = go(grad.at[row_slice((1 - core) * r2, r2)], half_in, 0, pc)
    yield
    first.wait_recv()
    base = core * r2

    def chip_sum(off):
        return grad[row_slice(base + off, 16), :] + half_in[row_slice(off, 16), :]

    away_a, away_b = (1 - xpos) * r8, r4 + (1 - ypos) * r8
    keep_a, keep_b = xpos * r8, r4 + ypos * r8

    def send_mid(i):
        mid[0, row_slice(i, 16), :] = chip_sum(away_a + i).astype(BF)
        mid[1, row_slice(i, 16), :] = chip_sum(away_b + i).astype(BF)
    chunked(r8, 16, send_mid)
    c_a = go(mid.at[0], mid.at[2], 1, px)
    c_b = go(mid.at[1], mid.at[3], 2, py)
    yield
    c_a.wait_recv()
    c_b.wait_recv()

    def two_sum(which, keep, off):
        return chip_sum(keep + off) + mid[2 + which, row_slice(off, 16), :].astype(F32)

    def send_last(i):
        last[0, row_slice(i, 16), :] = two_sum(0, keep_a, (1 - ypos) * r16 + i).astype(BF)
        last[1, row_slice(i, 16), :] = two_sum(1, keep_b, (1 - xpos) * r16 + i).astype(BF)
    chunked(r16, 16, send_last)
    c_a = go(last.at[0], last.at[2], 3, py)
    c_b = go(last.at[1], last.at[3], 4, px)
    yield
    c_a.wait_recv()
    c_b.wait_recv()
    pos_a, pos_b = base + keep_a + ypos * r16, base + keep_b + xpos * r16

    def total(i):
        out[row_slice(pos_a + i, 16), :] = (two_sum(0, keep_a, ypos * r16 + i) + last[2, row_slice(i, 16), :].astype(F32)).astype(BF)
        out[row_slice(pos_b + i, 16), :] = (two_sum(1, keep_b, xpos * r16 + i) + last[3, row_slice(i, 16), :].astype(F32)).astype(BF)
    chunked(r16, 16, total)
    sl_a, sl_b = out.at[row_slice(pos_a, r16)], out.at[row_slice(pos_b, r16)]
    c_a = go(sl_a, sl_a, 5, py)
    c_b = go(sl_b, sl_b, 6, px)
    yield
    c_a.wait_recv()
    c_b.wait_recv()
    sl_a, sl_b = out.at[row_slice(base + keep_a, r8)], out.at[row_slice(base + keep_b, r8)]
    c_a = go(sl_a, sl_a, 7, px)
    c_b = go(sl_b, sl_b, 8, py)
    yield
    c_a.wait_recv()
    c_b.wait_recv()
    sl = out.at[row_slice(base, r2)]
    c_c = go(sl, sl, 9, pc)
    yield
    c_c.wait_recv()
    for copy in sent:
        copy.wait_send()


def dot(lhs, rhs):
    return jnp.dot(lhs, rhs, preferred_element_type=F32)


def dot_rows(lhs, rhs):
    return lax.dot_general(lhs, rhs, (((0,), (0,)), ((), ())), preferred_element_type=F32)


def dot_cols(lhs, rhs):
    return lax.dot_general(lhs, rhs, (((1,), (1,)), ((), ())), preferred_element_type=F32)


def sigmoid(val):
    return 0.5 * jnp.tanh(0.5 * val) + 0.5


def pick(idx_col, size):
    ids = lax.broadcasted_iota(jnp.int32, (idx_col.shape[0], size), 1)
    return jnp.where(idx_col == ids, 1.0, 0.0).astype(BF)


def pick_t(idx_row, start, size):
    ids = lax.broadcasted_iota(jnp.int32, (size, idx_row.shape[1]), 0) + start
    return jnp.where(idx_row == ids, 1.0, 0.0).astype(BF)


def normalise(hidden, w_two, bias_two):
    out_lin = dot(hidden, w_two) + bias_two
    centered = out_lin - jnp.mean(out_lin, axis=-1, keepdims=True)
    inv_std = lax.rsqrt(jnp.mean(centered * centered, axis=-1, keepdims=True) + LN_EPS)
    return centered * inv_std, inv_std


def fold8(val):
    return jnp.sum(val.reshape(val.shape[0] // 8, 8, val.shape[1]), axis=0)


def layer_back(pre, sig, hidden, normed, inv_std, w_two, gamma, d_out, two_acc, vec_acc):
    d_normed = d_out * gamma
    d_lin = inv_std * (d_normed - jnp.mean(d_normed, axis=-1, keepdims=True)
                       - normed * jnp.mean(d_normed * normed, axis=-1, keepdims=True))
    d_lin_bf = d_lin.astype(BF)
    two_acc[...] += dot_rows(hidden, d_lin_bf)
    d_pre = dot_cols(d_lin_bf, w_two) * (sig * (1.0 + pre * (1.0 - sig)))
    vec_acc[0] += fold8(d_pre)
    vec_acc[1] += fold8(d_lin)
    vec_acc[2] += fold8(d_out * normed)
    vec_acc[3] += fold8(d_out)
    return d_pre.astype(BF)


def vec_block(vec_acc):
    rows = lax.broadcasted_iota(jnp.int32, (8, vec_acc.shape[2]), 0)
    out = jnp.zeros((8, vec_acc.shape[2]), F32)
    for j in range(4):
        out = jnp.where(rows == j, jnp.sum(vec_acc[j], axis=0, keepdims=True), out)
    return out


def tiles(first, last, tile, fn):
    def step(i, carry):
        fn(pl.multiple_of(i * tile, tile))
        return carry
    lax.fori_loop(first, last, step, 0)


TILE = 256
SLOTS = 192


def encode_body(grid_in, mesh_static, edge_static, send_col, w_grid_in, w_mesh_in, w_edge_in, w_grid_up, w_two, vec, d_grid_out,
                incoming, edge_lat, mesh_lat, grid_out, d_grid_part, grad_a, vec5,
                grid_lat, outgoing, vec_acc, sems):
    me = lax.axis_index(AXIS_NAME)
    barrier_signal()

    def embed(x_val, w_in, k):
        pre = dot(x_val, w_in[...]) + vec[k, 0:1, :]
        hidden = (pre * sigmoid(pre)).astype(BF)
        normed, _ = normalise(hidden, w_two[k], vec[k, 1:2, :])
        return (normed * vec[k, 2:3, :] + vec[k, 3:4, :]).astype(BF)

    def grid_tile(row):
        grid_lat[pl.ds(row, TILE), :] = embed(grid_in[pl.ds(row, TILE), :], w_grid_in, 0)
    tiles(0, grid_in.shape[0] // TILE, TILE, grid_tile)

    barrier_wait()
    copies = []
    for k in (6, 7, 2, 3, 4, 5, 1, 0):
        peer = flip(me, k)
        there = pl.ds(pl.multiple_of(peer * SLOTS, SLOTS), SLOTS)
        here = pl.ds(pl.multiple_of(me * SLOTS, SLOTS), SLOTS)
        rows = dot(pick(send_col[there, :], grid_lat.shape[0]), grid_lat[...]).astype(BF)
        if k == 0:
            incoming[here, :] = rows
        else:
            outgoing[there, :] = rows
            copy = remote(outgoing.at[there], incoming.at[here], sems, k, peer)
            copy.start()
            copies.append(copy)

    def edge_tile(row):
        edge_lat[pl.ds(row, TILE), :] = embed(edge_static[pl.ds(row, TILE), :], w_edge_in, 2)
    tiles(0, edge_static.shape[0] // TILE, TILE, edge_tile)
    mesh_lat[...] = embed(mesh_static[...], w_mesh_in, 1)

    grad_a[...] = jnp.zeros_like(grad_a)
    vec_acc[...] = jnp.zeros_like(vec_acc)
    two_acc, up_acc = grad_a.at[0:512], grad_a.at[512:1024]

    def cell_tile(row):
        lat = grid_lat[pl.ds(row, TILE), :]
        pre = dot(lat, w_grid_up[...]) + vec[5, 0:1, :]
        sig = sigmoid(pre)
        hidden = (pre * sig).astype(BF)
        normed, inv_std = normalise(hidden, w_two[5], vec[5, 1:2, :])
        upd = normed * vec[5, 2:3, :] + vec[5, 3:4, :]
        grid_out[pl.ds(row, TILE), :] = (lat.astype(F32) + upd).astype(BF)
        d_top = d_grid_out[pl.ds(row, TILE), :].astype(F32)
        d_pre = layer_back(pre, sig, hidden, normed, inv_std, w_two[5], vec[5, 2:3, :], d_top, two_acc, vec_acc)
        up_acc[...] += dot_rows(lat, d_pre)
        d_grid_part[pl.ds(row, TILE), :] = d_top + dot_cols(d_pre, w_grid_up[...])
    tiles(0, grid_in.shape[0] // TILE, TILE, cell_tile)
    vec5[...] = vec_block(vec_acc)
    for copy in copies:
        copy.wait()


def update_body(incoming, edge_lat, mesh_lat, idx_col, src_row, dst_row, send_row, edge_static, edge_static_t, mesh_static, mesh_static_t, grid_in,
                w_grid_in, w_mesh_in, w_edge_in, w_edge_up, w_mesh_up, w_two, vec, d_mesh_out, d_grid_part, grad_a, vec5,
                mesh_out, d_grid_in, sum_a, sum_b, sum_c, sum_e, sum_d,
                pre3, normed3, inv3, d_pre3, d_slot, d_incoming, d_outgoing, agg, d_node, d_mesh, d_agg, vec_acc,
                grad_b, grad_c, half_a, half_b, mid_a, mid_b, mid_c, mid_e, mid_d, last_a, last_b, last_c, last_e, last_d,
                sem_a, sem_b, sem_c, sem_e, sem_d, sems):
    me = lax.axis_index(AXIS_NAME)
    n_edge, n_grid, n_mesh, n_slot = edge_lat.shape[0], grid_in.shape[0], mesh_lat.shape[0], incoming.shape[0]
    grad_e, grad_d = normed3.at[0:1024], normed3.at[1024:2048]
    half_c, half_e, half_d = pre3.at[0:1024], pre3.at[1024:1536], pre3.at[1536:2048]
    up_edge, up_send, up_recv = w_edge_up.at[0:512], w_edge_up.at[512:1024], w_edge_up.at[1024:1536]
    node_self, node_agg = w_mesh_up.at[0:512], w_mesh_up.at[512:1024]
    live = []

    def advance():
        for gen in list(live):
            try:
                next(gen)
            except StopIteration:
                live.remove(gen)

    def begin(*args):
        gen = reduce_steps(*args)
        next(gen)
        live.append(gen)

    def groups(count, fn):
        for g in range(3):
            tiles(g * count // 3, (g + 1) * count // 3, TILE, fn)
            advance()

    barrier_signal()
    barrier_wait()
    begin(grad_a, sum_a, half_a, mid_a, last_a, sem_a)
    agg[...] = jnp.zeros_like(agg)

    def edge_forward(row):
        here = pl.ds(row, TILE)
        lat = edge_lat[here, :]
        sender = dot(pick(idx_col[here, 0:1], n_slot), incoming[...]).astype(BF)
        receiver = dot(pick(idx_col[here, 1:2], n_mesh), mesh_lat[...]).astype(BF)
        pre = dot(jnp.concatenate([lat, sender, receiver], axis=1), w_edge_up[...]) + vec[3, 0:1, :]
        hidden = (pre * sigmoid(pre)).astype(BF)
        normed, inv_std = normalise(hidden, w_two[3], vec[3, 1:2, :])
        pre3[here, :] = pre
        normed3[here, :] = normed
        inv3[here, :] = inv_std
        edge_new = (lat.astype(F32) + normed * vec[3, 2:3, :] + vec[3, 3:4, :]).astype(BF)
        agg[...] += dot(pick_t(dst_row[:, here], 0, n_mesh), edge_new)
    groups(n_edge // TILE, edge_forward)

    def clear_vec():
        vec_acc[...] = jnp.zeros_like(vec_acc)

    grad_b[...] = jnp.zeros_like(grad_b)
    clear_vec()
    lat = mesh_lat[...]
    agg_bf = agg[...].astype(BF)
    pre = dot(jnp.concatenate([lat, agg_bf], axis=1), w_mesh_up[...]) + vec[4, 0:1, :]
    sig = sigmoid(pre)
    hidden = (pre * sig).astype(BF)
    normed, inv_std = normalise(hidden, w_two[4], vec[4, 1:2, :])
    mesh_out[...] = (lat.astype(F32) + normed * vec[4, 2:3, :] + vec[4, 3:4, :]).astype(BF)
    d_top = d_mesh_out[...].astype(F32)
    d_pre = layer_back(pre, sig, hidden, normed, inv_std, w_two[4], vec[4, 2:3, :], d_top, grad_b.at[1024:1536], vec_acc)
    grad_b[0:512, :] = dot_rows(lat, d_pre)
    grad_b[512:1024, :] = dot_rows(agg_bf, d_pre)
    d_mesh[...] = d_top + dot_cols(d_pre, node_self[...])
    d_agg[...] = dot_cols(d_pre, node_agg[...]).astype(BF)
    vec4 = vec_block(vec_acc)
    advance()
    begin(grad_b, sum_b, half_b, mid_b, last_b, sem_b)

    clear_vec()
    d_node[...] = jnp.zeros_like(d_node)
    grad_c[...] = jnp.zeros_like(grad_c)

    def edge_backward(row):
        here = pl.ds(row, TILE)
        d_out = dot(pick(idx_col[here, 1:2], n_mesh), d_agg[...])
        pre = pre3[here, :]
        sig = sigmoid(pre)
        hidden = (pre * sig).astype(BF)
        d_pre = layer_back(pre, sig, hidden, normed3[here, :], inv3[here, :], w_two[3], vec[3, 2:3, :], d_out, grad_c.at[1536:2048], vec_acc)
        d_pre3[here, :] = d_pre
        d_node[...] += dot(pick_t(dst_row[:, here], 0, n_mesh), d_pre)
        grad_c[0:512, :] += dot_rows(edge_lat[here, :], d_pre)
    groups(n_edge // TILE, edge_backward)
    vec3 = vec_block(vec_acc)

    copies = []
    for k in (1, 6, 7, 2, 3, 4, 5, 0):
        peer = flip(me, k)
        start = pl.multiple_of(peer * SLOTS, SLOTS)
        there, here = pl.ds(start, SLOTS), pl.ds(pl.multiple_of(me * SLOTS, SLOTS), SLOTS)
        slot = dot(pick_t(src_row[...], start, SLOTS), d_pre3[...]).astype(BF)
        d_slot[there, :] = slot
        back = dot_cols(slot, up_send[...]).astype(BF)
        if k == 0:
            d_outgoing[here, :] = back
        else:
            d_incoming[there, :] = back
            copy = remote(d_incoming.at[there], d_outgoing.at[here], sems, k, peer)
            copy.start()
            copies.append(copy)
    advance()

    def slot_tile(row):
        here = pl.ds(row, TILE)
        grad_c[512:1024, :] += dot_rows(incoming[here, :], d_slot[here, :])
    tiles(0, n_slot // TILE, TILE, slot_tile)
    d_node_bf = d_node[...].astype(BF)
    grad_c[1024:1536, :] = dot_rows(lat, d_node_bf)
    d_mesh_full = d_mesh[...] + dot_cols(d_node_bf, up_recv[...])
    copies[0].wait_recv()
    begin(grad_c, sum_c, half_c, mid_c, last_c, sem_c)

    grad_e[...] = jnp.zeros_like(grad_e)
    grad_d[...] = jnp.zeros_like(grad_d)

    def recompute(x_val, w_in, k):
        pre = dot(x_val, w_in[...]) + vec[k, 0:1, :]
        sig = sigmoid(pre)
        hidden = (pre * sig).astype(BF)
        normed, inv_std = normalise(hidden, w_two[k], vec[k, 1:2, :])
        return pre, sig, hidden, normed, inv_std, w_two[k], vec[k, 2:3, :]

    clear_vec()
    d_pre = layer_back(*recompute(mesh_static[...], w_mesh_in, 1), d_mesh_full, grad_e.at[512:1024], vec_acc)
    grad_d[832:840, :] = dot(mesh_static_t[...], d_pre)[0:8, :]
    grad_d[792:800, :] = vec_block(vec_acc)
    clear_vec()

    def edge_embed_back(row):
        here = pl.ds(row, TILE)
        d_out = dot(pick(idx_col[here, 1:2], n_mesh), d_agg[...]) + dot_cols(d_pre3[here, :], up_edge[...])
        d_pre = layer_back(*recompute(edge_static[here, :], w_edge_in, 2), d_out, grad_e.at[0:512], vec_acc)
        grad_d[840:848, :] += dot(edge_static_t[:, here], d_pre)[0:8, :]
    groups(n_edge // TILE, edge_embed_back)
    grad_d[800:808, :] = vec_block(vec_acc)
    grad_d[808:816, :] = vec3
    grad_d[816:824, :] = vec4
    grad_d[824:832, :] = vec5[...]
    begin(grad_e, sum_e, half_e, mid_e, last_e, sem_e)

    for copy in copies[1:]:
        copy.wait_recv()
    clear_vec()

    def grid_back(row):
        here = pl.ds(row, TILE)
        x_val = grid_in[here, :]
        d_out = d_grid_part[here, :] + dot(pick_t(send_row[...], row, TILE), d_outgoing[...])
        d_pre = layer_back(*recompute(x_val, w_grid_in, 0), d_out, grad_d.at[0:512], vec_acc)
        grad_d[512:784, :] += dot_rows(x_val, d_pre)
        d_grid_in[here, :] = dot_cols(d_pre, w_grid_in[...])
    groups(n_grid // TILE, grid_back)
    grad_d[784:792, :] = vec_block(vec_acc)
    begin(grad_d, sum_d, half_d, mid_d, last_d, sem_d)
    while live:
        advance()
    for copy in copies:
        copy.wait_send()


def shape(rows, cols, dtype):
    return jax.ShapeDtypeStruct((rows, cols), dtype)


def solution(mesh):
    row_spec = P(AXIS_NAME, None)
    edge_spec = P(AXIS_NAME)
    rep_spec = P()
    in_specs = (row_spec, row_spec, row_spec, row_spec, edge_spec, edge_spec) + (rep_spec,) * 8 + (row_spec, row_spec)
    out_specs = (row_spec, row_spec, row_spec) + (rep_spec,) * 8
    vm = pl.BlockSpec(memory_space=pltpu.VMEM)

    def local_step(grid_in, mesh_static, edge_static, send_rows, edge_src, edge_dst, w_grid_in, w_mesh_in, w_edge_in, w_edge_up, w_mesh_up, w_grid_up, w_second, vectors, d_mesh_out, d_grid_out):
        latent = w_grid_up.shape[0]
        n_grid, n_mesh, n_edge, n_slot = grid_in.shape[0], mesh_static.shape[0], edge_src.shape[0], send_rows.size
        f_dim, m_dim, e_dim = w_grid_in.shape[0], w_mesh_in.shape[0], w_edge_in.shape[0]
        idx_col = jnp.stack([edge_src, edge_dst], axis=1)
        send_flat = send_rows.reshape(-1)

        def call(body, ins, outs, scratch, name, ident):
            return pl.pallas_call(
                body, out_shape=outs, in_specs=[vm] * len(ins), out_specs=[vm] * len(outs), scratch_shapes=scratch, name=name,
                compiler_params=pltpu.CompilerParams(collective_id=ident, has_side_effects=True, vmem_limit_bytes=67043328),
            )(*ins)

        incoming, edge_lat, mesh_lat, grid_out, d_grid_part, grad_a, vec5 = call(
            encode_body,
            (grid_in, mesh_static, edge_static, send_flat[:, None], w_grid_in, w_mesh_in, w_edge_in, w_grid_up, w_second, vectors, d_grid_out),
            [shape(n_slot, latent, BF), shape(n_edge, latent, BF), shape(n_mesh, latent, BF), shape(n_grid, latent, BF),
             shape(n_grid, latent, F32), shape(1024, latent, F32), shape(8, latent, F32)],
            [pltpu.VMEM((n_grid, latent), BF), pltpu.VMEM((n_slot, latent), BF), pltpu.VMEM((4, 8, latent), F32), pltpu.SemaphoreType.DMA((2, 8))],
            'encode', 0)

        r_a, r_b, r_c, r_e, r_d = 1024, 1536, 2048, 1024, 1024
        vmem = lambda rows, dtype: pltpu.VMEM((rows, latent), dtype)
        scratch = [vmem(n_edge, F32), vmem(n_edge, F32), pltpu.VMEM((n_edge, 1), F32), vmem(n_edge, BF), vmem(n_slot, BF), vmem(n_slot, BF), vmem(n_slot, BF),
                   vmem(n_mesh, F32), vmem(n_mesh, F32), vmem(n_mesh, F32), vmem(n_mesh, BF), pltpu.VMEM((4, 8, latent), F32),
                   vmem(r_b, F32), vmem(r_c, F32), vmem(r_a // 2, F32), vmem(r_b // 2, F32)]
        scratch += [pltpu.VMEM((4, r // 8, latent), BF) for r in (r_a, r_b, r_c, r_e, r_d)]
        scratch += [pltpu.VMEM((4, r // 16, latent), BF) for r in (r_a, r_b, r_c, r_e, r_d)]
        scratch += [pltpu.SemaphoreType.DMA((2, 10))] * 5 + [pltpu.SemaphoreType.DMA((2, 8))]
        pad_t = lambda val: jnp.pad(val.T, ((0, 16 - val.shape[1]), (0, 0)))
        mesh_out, d_grid_in, s_a, s_b, s_c, s_e, s_d = call(
            update_body,
            (incoming, edge_lat, mesh_lat, idx_col, edge_src[None, :], edge_dst[None, :], send_flat[None, :], edge_static, pad_t(edge_static),
             mesh_static, pad_t(mesh_static), grid_in, w_grid_in, w_mesh_in, w_edge_in, w_edge_up, w_mesh_up, w_second, vectors,
             d_mesh_out, d_grid_part, grad_a, vec5),
            [shape(n_mesh, latent, BF), shape(n_grid, f_dim, F32)] + [shape(r, latent, BF) for r in (r_a, r_b, r_c, r_e, r_d)],
            scratch, 'update', 1)

        o_v = latent + f_dim
        two = jnp.stack([s_d[:latent], s_e[latent:], s_e[:latent], s_c[3 * latent:], s_b[2 * latent:], s_a[:latent]]).astype(F32)
        vec = s_d[o_v:o_v + 48].reshape(6, 8, latent)[:, :4].astype(F32)
        return (mesh_out, grid_out, d_grid_in, s_d[latent:o_v].astype(F32), s_d[o_v + 48:o_v + 48 + m_dim].astype(F32),
                s_d[o_v + 56:o_v + 56 + e_dim].astype(F32), s_c[:3 * latent].astype(F32), s_b[:2 * latent].astype(F32),
                s_a[latent:].astype(F32), two, vec)

    return jax.shard_map(local_step, mesh=mesh, in_specs=in_specs, out_specs=out_specs, check_vma=False)
```
